512 devices in a mesh: vrow: 32 (over z_hi, x, y), aux: 8 (over z_lo), grp: 2 (over core).
Axes of the slice: x: 4, y: 4, z: 16 (z_hi: 2, z_lo: 8; z = z_hi * 8 + z_lo), core: 2. Of those that a mesh axis runs over, the one named last changes fastest.
Arguments:
- trials: bfloat16 [192, 3840], P(None, 'vrow'), may hold values from -6 to 6
- vv_factors: bfloat16 [64, 3840, 3840], P(('aux', 'grp'), 'vrow'), may hold values from -0.09375 to 0.09375
- screened: bfloat16 [64, 96, 96], P(('aux', 'grp')), may hold values from -0.078125 to 0.078125
- ov_factors: bfloat16 [64, 3840, 96], P(('aux', 'grp'), 'vrow'), may hold values from -0.0625 to 0.0625
- occ_energy: float32 [96], replicated, may hold values from -1.5 to -0.3
- virt_energy: float32 [3840], replicated, may hold values from 0.2 to 2.5
- occ_order: int32 [96], replicated, may hold values from 0 to 95, each once
- virt_order: int32 [3840], P('vrow'), may hold values from 0 to 3839, each once
Outputs:
- sigma: float32 [192, 3840], P(('aux', 'grp'), 'vrow')
The draws below stay inside these ranges and needn't reach their ends.
Inputs may be any that keep to these rules, and one draw needn't show every extreme that they name: `occ_order`: each active occupied orbital names a different entry. `virt_order`: each virtual orbital names a different entry.
All inputs are finite; a program needn't handle non-finite values.
Results may differ from the reference program's by a relative error of at most 0.0022.
Values may be sent and summed in bfloat16 or wider, within the bound.
No kernel may reach another device: no remote copies, remote signals or barrier semaphores. Data moves between devices by JAX's collectives and lax.ppermute only.
A program may use at most 64 MiB of HBM per device.

```python
import jax
import jax.numpy as jnp
from jax import lax

NO = 96
NV = 3840
NTR = 2
WIN = 64


def shard_levels(key, extent, shards, low, largest):
    factor_of = 1.0
    for dim, parts in shards:
        heights = jax.random.uniform(jax.random.fold_in(jax.random.fold_in(key, 6), dim), (parts,), jnp.float32, low / len(shards), largest / len(shards))
        factor_of = factor_of * jnp.repeat(jnp.exp(heights), extent[dim] // parts).reshape((-1,) + (1,) * (len(extent) - 1 - dim))
    return factor_of


def gaussian(rng, dims, scale, limit, split=(), held_as=jnp.bfloat16):
    level = shard_levels(rng, dims, split, -0.22, 0.18) if split else 1.0
    drawn = jax.random.normal(rng, dims, jnp.float32) * scale * level
    return jnp.minimum(jnp.maximum(drawn, -limit), limit).astype(held_as)


def setup_inputs(seed: int = 0) -> dict:
    key_of = jax.random.split(jax.random.key(seed), 9)
    trials = gaussian(key_of[0], (NTR * NO, NV), 1.0, 6.0, ((1, 32),))
    vv_factors = gaussian(key_of[1], (WIN, NV, NV), NV ** -0.5, 0.09375, ((0, 16), (1, 32)))
    screened = gaussian(key_of[2], (WIN, NO, NO), (NO * WIN) ** -0.5, 0.078125, ((0, 16),))
    ov_factors = gaussian(key_of[3], (WIN, NV, NO), (2 * (WIN * NO * NV) ** 0.5) ** -0.5, 0.0625, ((0, 16), (1, 32)))
    occ_energy = jnp.clip(jax.random.uniform(key_of[4], (NO,), jnp.float32, -1.5, -0.3), -1.5, -0.3)
    virt_energy = jnp.clip(jax.random.uniform(key_of[5], (NV,), jnp.float32, 0.2, 2.5), 0.2, 2.5)
    occ_order = jax.random.permutation(key_of[6], NO).astype(jnp.int32)
    virt_order = jax.random.permutation(key_of[7], NV).astype(jnp.int32)
    return {"trials": trials, "vv_factors": vv_factors, "screened": screened, "ov_factors": ov_factors, "occ_energy": occ_energy, "virt_energy": virt_energy, "occ_order": occ_order, "virt_order": virt_order}


def reference(trials, vv_factors, screened, ov_factors, occ_energy, virt_energy, occ_order, virt_order):
    occupied = occ_energy.shape[0]
    count_trials = trials.shape[0] // occupied
    trials_wide = trials.astype(jnp.float32)
    split_trials = trials_wide.reshape(count_trials, occupied, NV)
    factors_wide = ov_factors.astype(jnp.float32)
    pair_sums = jnp.einsum("qai,tia->qt", factors_wide, split_trials)
    exchange_term = 2.0 * jnp.einsum("qai,qt->tia", factors_wide, pair_sums)

    def add_function(running, inputs):
        factor_slab, screen = inputs
        product = jnp.dot(trials, factor_slab.T, preferred_element_type=jnp.float32).astype(jnp.bfloat16)
        shaped = product.astype(jnp.float32).reshape(count_trials, occupied, NV)
        return running + jnp.einsum("ji,tja->tia", screen.astype(jnp.float32), shaped), None

    direct_term, unused = lax.scan(add_function, jnp.zeros((count_trials, occupied, NV), jnp.float32), (vv_factors, screened))
    virt_levels = virt_energy[virt_order.astype(jnp.int32)]
    occ_levels = occ_energy[occ_order.astype(jnp.int32)]
    differences = virt_levels[None, :] - jnp.tile(occ_levels, count_trials)[:, None]
    combined = (exchange_term - direct_term).reshape(count_trials * occupied, NV)
    return differences * trials_wide + combined
```

```python
import functools

import jax
import jax.numpy as jnp
from jax import lax
from jax.experimental import pallas as pl
from jax.experimental.pallas import tpu as pltpu
from jax.sharding import Mesh
from jax.sharding import PartitionSpec as P

VROW = ("half", "x", "y")
PLANE = ("x", "y")
WINDOW = ("aux", "grp")
LANES = 128


def vmem():
    return pl.BlockSpec(memory_space=pltpu.VMEM)


def pack_kernel(trials_ref, ov_ref, block_ref):
    core = lax.axis_index("grp")
    row = (lax.axis_index("half") * lax.axis_size("x") + lax.axis_index("x")) * lax.axis_size("y") + lax.axis_index("y")
    functions, occupied, virt = ov_ref.shape
    count = trials_ref.shape[0] // occupied
    spare = LANES - virt
    split = [trials_ref[pl.ds(t * occupied, occupied), :].astype(jnp.float32) for t in range(count)]
    sums = []
    for q in range(functions):
        factors = ov_ref[q].astype(jnp.float32)
        for t in range(count):
            sums.append(jnp.sum(factors * split[t], axis=0, keepdims=True))
    sums = jnp.sum(jnp.concatenate(sums, axis=0), axis=1, keepdims=True)
    pieces = []
    rest = sums
    for _ in range(3):
        piece = rest.astype(jnp.bfloat16).astype(jnp.float32)
        pieces.append(piece)
        rest = rest - piece
    carried = 3 * sums.shape[0]
    column = jnp.concatenate([*pieces, jnp.zeros((occupied - carried, 1), jnp.float32)], axis=0)
    own = jnp.where(core == 0, split[0], split[1])
    wide = jnp.concatenate([own, jnp.broadcast_to(column, (occupied, spare))], axis=1)
    turn = lax.rem(row * virt, LANES)
    block_ref[...] = pltpu.roll(wide, turn, 1).astype(jnp.bfloat16)


def term_kernel(near_ref, far_ref, vv_ref, vv_peer_ref, screened_ref, screened_peer_ref, ov_ref, out_ref, whole_ref):
    core = lax.axis_index("grp")
    half = lax.axis_index("half")
    functions, occupied, virt = ov_ref.shape
    count = 2
    blocks = near_ref.shape[0]
    spare = LANES - virt
    tiles = blocks * virt // LANES
    carried = 3 * functions * count
    lanes = lax.broadcasted_iota(jnp.int32, (occupied, LANES), 1)
    few = lax.broadcasted_iota(jnp.int32, (carried, LANES), 1)
    gathered = jnp.zeros((carried, LANES), jnp.float32)

    for side, ref in enumerate((near_ref, far_ref)):
        start = jnp.where(half == side, 0, tiles * LANES)
        held = ref[0].astype(jnp.float32)
        for j in range(blocks):
            free = virt - spare * j
            picked = (few >= free) & (few < free + spare)
            gathered = gathered + jnp.where(picked, held[:carried], 0.0)
            if j < tiles:
                after = ref[j + 1].astype(jnp.float32)
                tile = jnp.where(lanes < free, held, after).astype(jnp.bfloat16)
                whole_ref[:, pl.ds(pl.multiple_of(start + j * LANES, LANES), LANES)] = tile
                held = after

    pair = jnp.sum(gathered, axis=1, keepdims=True) * (1.0 / spare)
    entries = functions * count
    pair = pair[:entries] + pair[entries : 2 * entries] + pair[2 * entries :]

    mine = jnp.zeros((occupied, virt), jnp.float32)
    other = jnp.zeros((occupied, virt), jnp.float32)
    for q in range(functions):
        factors = ov_ref[q].astype(jnp.float32)
        first = pair[q * count : q * count + 1]
        second = pair[q * count + 1 : q * count + 2]
        mine = mine + factors * jnp.where(core == 0, first, second)
        other = other + factors * jnp.where(core == 0, second, first)

    whole = whole_ref[...]
    turned = jnp.zeros((virt, occupied), jnp.float32)
    for q in range(functions):
        for factor, screen in ((vv_ref, screened_ref), (vv_peer_ref, screened_peer_ref)):
            image = lax.dot_general(factor[q], whole, (((1,), (1,)), ((), ())), preferred_element_type=jnp.float32)
            turned = turned + jnp.dot(image.astype(jnp.bfloat16), screen[q], preferred_element_type=jnp.float32)

    mine = 2.0 * mine - turned.T
    other = 2.0 * other
    share = out_ref.shape[1]
    per = occupied // share
    for m in range(per):
        out_ref[core * per + m] = mine[m * share : (m + 1) * share].astype(out_ref.dtype)
        out_ref[(1 - core) * per + m] = other[m * share : (m + 1) * share].astype(out_ref.dtype)


def table_lookup(order, table):
    columns = lax.broadcasted_iota(jnp.int32, (order.shape[0], table.shape[0]), 1)
    picker = (order[:, None] == columns).astype(jnp.float32)
    return jnp.dot(picker, table, precision=lax.Precision.HIGHEST)


def swapped(value, axis):
    return lax.ppermute(value, axis, [(0, 1), (1, 0)])


def on_device(trials, vv_factors, screened, ov_factors, occ_energy, virt_energy, occ_order, virt_order):
    groups = lax.axis_size(WINDOW)
    rows_all, virt = trials.shape
    occupied = occ_energy.shape[0]
    functions = vv_factors.shape[0]
    row_share = rows_all // groups
    row_offset = lax.axis_index(WINDOW) * row_share
    ov_rows = jnp.swapaxes(ov_factors, 1, 2)
    peers = lax.axis_size(PLANE)

    block = pl.pallas_call(
        pack_kernel,
        out_shape=jax.ShapeDtypeStruct((occupied, LANES), jnp.bfloat16),
        in_specs=[vmem(), vmem()],
        out_specs=vmem(),
        compiler_params=pltpu.CompilerParams(vmem_limit_bytes=4 << 20),
        name="pack",
    )(trials, ov_rows)

    far = swapped(block, "half")
    vv_peer = swapped(vv_factors, "grp")
    screened_peer = swapped(screened, "grp")

    both = jnp.broadcast_to(jnp.stack([block, far])[None], (peers, 2, occupied, LANES))
    both = lax.all_to_all(both, PLANE, 0, 0, tiled=True)

    flops = 2 * 2 * functions * virt * vv_factors.shape[2] * occupied
    terms = pl.pallas_call(
        term_kernel,
        out_shape=jax.ShapeDtypeStruct((groups, row_share, virt), jnp.bfloat16),
        in_specs=[vmem()] * 7,
        out_specs=vmem(),
        scratch_shapes=[pltpu.VMEM((occupied, vv_factors.shape[2]), jnp.bfloat16)],
        compiler_params=pltpu.CompilerParams(vmem_limit_bytes=24 << 20),
        cost_estimate=pl.CostEstimate(flops=flops, bytes_accessed=8 << 20, transcendentals=0),
        name="terms",
    )(both[:, 0], both[:, 1], vv_factors, vv_peer, screened, screened_peer, ov_rows)

    terms = lax.all_to_all(terms, WINDOW, 0, 0, tiled=True)
    summed = terms.astype(jnp.float32).sum(axis=0)

    virt_levels = table_lookup(virt_order, virt_energy)
    occ_levels = table_lookup(occ_order, occ_energy)
    row_ids = row_offset + lax.broadcasted_iota(jnp.int32, (row_share,), 0)
    row_levels = table_lookup(row_ids % occupied, occ_levels)
    own_trials = lax.dynamic_slice_in_dim(trials, row_offset, row_share, 0).astype(jnp.float32)
    return summed + (virt_levels[None, :] - row_levels[:, None]) * own_trials


def solution(mesh):
    torus = Mesh(
        mesh.devices.reshape(2, 4, 4, mesh.shape["aux"], mesh.shape["grp"]),
        ("half", "x", "y", "aux", "grp"),
    )
    placed = (
        P(None, VROW),
        P(WINDOW, VROW, None),
        P(WINDOW, None, None),
        P(WINDOW, VROW, None),
        P(),
        P(),
        P(),
        P(VROW),
    )
    return jax.shard_map(on_device, mesh=torus, in_specs=placed, out_specs=P(WINDOW, VROW), check_vma=False)
```

```python
import jax
import jax.numpy as jnp
from jax import lax
from jax.experimental import pallas as pl
from jax.experimental.pallas import tpu as pltpu
from jax.sharding import Mesh
from jax.sharding import PartitionSpec as P

VROW = ("half", "x", "y")
PLANE = ("x", "y")
WINDOW = ("aux", "grp")
LANES = 128
ROWS = 128
PIECES = 3


def vmem():
    return pl.BlockSpec(memory_space=pltpu.VMEM)


def hbm():
    return pl.BlockSpec(memory_space=pltpu.HBM)


def in_pieces(values):
    pieces = []
    for _ in range(PIECES):
        piece = values.astype(jnp.bfloat16).astype(jnp.float32)
        pieces.append(piece)
        values = values - piece
    return pieces


def window_order(count):
    chips = count // 2
    middle = sorted(range(chips), key=lambda a: abs(2 * a + 1 - chips))
    listed = []
    for k in range(0, chips, 2):
        pair = middle[k : k + 2]
        listed += [2 * a + 1 for a in pair] + [2 * a for a in pair]
    return listed


def plane_order(count):
    first = 2 * count // 3
    return [first, *(place for place in range(count) if place != first)]


def pack_kernel(trials_hbm, ov_hbm, screened_hbm, block_ref, ov_ref, screened_ref, trials_ref, sems):
    copies = [
        pltpu.make_async_copy(trials_hbm, trials_ref, sems.at[0]),
        pltpu.make_async_copy(ov_hbm, ov_ref, sems.at[1]),
        pltpu.make_async_copy(screened_hbm, screened_ref, sems.at[2]),
    ]
    for copy in copies:
        copy.start()
    for copy in copies[:2]:
        copy.wait()
    core = lax.axis_index("grp")
    row = (lax.axis_index("half") * lax.axis_size("x") + lax.axis_index("x")) * lax.axis_size("y") + lax.axis_index("y")
    functions, occupied, virt = ov_ref.shape
    count = trials_ref.shape[0] // occupied
    spare = LANES - virt
    split = [trials_ref[pl.ds(t * occupied, occupied), :].astype(jnp.float32) for t in range(count)]
    factors = [ov_ref[q].astype(jnp.float32) for q in range(functions)]
    sums = [jnp.sum(factors[q] * split[t], axis=0, keepdims=True) for t in range(count) for q in range(functions)]
    sums = jnp.sum(jnp.concatenate(sums, axis=0), axis=1, keepdims=True)
    carried = PIECES * sums.shape[0]
    column = jnp.concatenate([*in_pieces(sums), jnp.zeros((occupied - carried, 1), jnp.float32)], axis=0)
    own = jnp.where(core == 0, split[0], split[1])
    wide = jnp.concatenate([own, jnp.broadcast_to(column, (occupied, spare))], axis=1)
    turn = lax.rem(row * virt, LANES)
    block_ref[...] = pltpu.roll(wide, turn, 1).astype(jnp.bfloat16)
    copies[2].wait()


def term_kernel(
    plane, window, both_ref, vv_hbm, vv_peer_hbm, screened_ref, screened_peer_ref, ov_ref, out_ref, whole_ref, held_ref, sems
):
    core = lax.axis_index("grp")
    half = lax.axis_index("half")
    functions, occupied, virt = ov_ref.shape
    copies = [
        [
            pltpu.make_async_copy(
                source.at[q],
                held_ref.at[pl.ds((side * functions + q) * ROWS, virt), :],
                sems.at[side * functions + q],
            )
            for q in range(functions)
        ]
        for side, source in enumerate((vv_hbm, vv_peer_hbm))
    ]
    for side in copies:
        for copy in side:
            copy.start()

    blocks = both_ref.shape[0]
    spare = LANES - virt
    tiles = blocks * virt // LANES
    entries = out_ref.shape[0] * out_ref.shape[1] // occupied * functions
    lanes = lax.broadcasted_iota(jnp.int32, (occupied, LANES), 1)
    few = lax.broadcasted_iota(jnp.int32, (PIECES * entries, LANES), 1)
    gathered = jnp.zeros((PIECES * entries, LANES), jnp.float32)
    for side in range(2):
        start = jnp.where(half == side, 0, tiles * LANES)
        held = both_ref[plane.index(0), side].astype(jnp.float32)
        for j in range(blocks):
            free = virt - spare * j
            picked = (few >= free) & (few < free + spare)
            gathered = gathered + jnp.where(picked, held[: PIECES * entries], 0.0)
            if j < tiles:
                after = both_ref[plane.index(j + 1), side].astype(jnp.float32)
                tile = jnp.where(lanes < free, held, after).astype(jnp.bfloat16)
                whole_ref[:, pl.ds(pl.multiple_of(start + j * LANES, LANES), LANES)] = tile
                held = after
    pair = jnp.sum(gathered, axis=1, keepdims=True) * (2.0 / spare)
    pair = sum(pair[k * entries : (k + 1) * entries] for k in range(PIECES))

    mine = jnp.zeros((occupied, virt), jnp.float32)
    other = jnp.zeros((occupied, virt), jnp.float32)
    for q in range(functions):
        factors = ov_ref[q].astype(jnp.float32)
        first, second = pair[q : q + 1], pair[functions + q : functions + q + 1]
        mine = mine + factors * jnp.where(core == 0, first, second)
        other = other + factors * jnp.where(core == 0, second, first)

    turned = jnp.zeros((virt, occupied), jnp.float32)
    for side, screen in enumerate((screened_ref, screened_peer_ref)):
        for copy in copies[side]:
            copy.wait()
        factor = held_ref[pl.ds(side * functions * ROWS, functions * ROWS), :]
        image = lax.dot_general(factor, whole_ref[...], (((1,), (1,)), ((), ())), preferred_element_type=jnp.float32)
        image = image.astype(jnp.bfloat16)
        for q in range(functions):
            turned = turned + jnp.dot(
                image[q * ROWS : q * ROWS + virt], screen[q], preferred_element_type=jnp.float32
            )
    mine = mine - turned.T

    share = out_ref.shape[1]
    per = occupied // share
    places = [window.index(w) for w in range(len(window))]
    for m in range(per):
        low, high = places[m], places[per + m]
        rows = slice(m * share, (m + 1) * share)
        out_ref[jnp.where(core == 0, low, high)] = mine[rows].astype(out_ref.dtype)
        out_ref[jnp.where(core == 0, high, low)] = other[rows].astype(out_ref.dtype)


def finish_kernel(terms_ref, base_ref, out_ref):
    total = base_ref[...]
    for place in range(terms_ref.shape[0]):
        total = total + terms_ref[place].astype(jnp.float32)
    out_ref[...] = total


def table_lookup(order, table):
    columns = lax.broadcasted_iota(jnp.int32, (order.shape[0], table.shape[0]), 1)
    picker = (order[:, None] == columns).astype(jnp.float32)
    return jnp.dot(picker, table, precision=lax.Precision.HIGHEST)


def level_part(trials, occ_energy, virt_energy, occ_order, virt_order, row_offset, row_share):
    occupied = occ_energy.shape[0]
    virt_levels = table_lookup(virt_order, virt_energy)
    occ_levels = table_lookup(occ_order, occ_energy)
    row_ids = row_offset + lax.broadcasted_iota(jnp.int32, (row_share,), 0)
    row_levels = table_lookup(row_ids % occupied, occ_levels)
    own_trials = lax.dynamic_slice_in_dim(trials, row_offset, row_share, 0).astype(jnp.float32)
    return (virt_levels[None, :] - row_levels[:, None]) * own_trials


def on_device(trials, vv_factors, screened, ov_factors, occ_energy, virt_energy, occ_order, virt_order):
    groups = lax.axis_size(WINDOW)
    rows_all, virt = trials.shape
    occupied = occ_energy.shape[0]
    functions, _, virt_all = vv_factors.shape
    row_share = rows_all // groups
    row_offset = lax.axis_index(WINDOW) * row_share
    ov_rows = jnp.swapaxes(ov_factors, 1, 2)
    peers = lax.axis_size(PLANE)
    window = window_order(groups)
    plane = plane_order(peers)
    cores = [(0, 1), (1, 0)]

    block, ov_held, screened_held = pl.pallas_call(
        pack_kernel,
        out_shape=(
            jax.ShapeDtypeStruct((occupied, LANES), jnp.bfloat16),
            jax.ShapeDtypeStruct(ov_rows.shape, jnp.bfloat16),
            jax.ShapeDtypeStruct(screened.shape, jnp.bfloat16),
        ),
        in_specs=[hbm()] * 3,
        out_specs=(vmem(),) * 3,
        scratch_shapes=[pltpu.VMEM(trials.shape, jnp.bfloat16), pltpu.SemaphoreType.DMA((3,))],
        compiler_params=pltpu.CompilerParams(vmem_limit_bytes=54960 << 10),
        name="pack",
    )(trials, ov_rows, screened)

    far = lax.ppermute(block, "half", cores)
    screened_peer = lax.ppermute(screened_held, "grp", cores)
    vv_peer = lax.ppermute(vv_factors, "grp", cores)

    far, screened_peer = lax.optimization_barrier((far, screened_peer))
    both = jnp.broadcast_to(jnp.stack([block, far])[None], (peers, 2, occupied, LANES))
    both = lax.all_to_all(both, PLANE, 0, 0, tiled=True, axis_index_groups=[plane])

    flops = 2 * 2 * functions * virt * virt_all * occupied
    terms = pl.pallas_call(
        lambda *refs: term_kernel(plane, window, *refs),
        out_shape=jax.ShapeDtypeStruct((groups, row_share, virt), jnp.bfloat16),
        in_specs=[vmem(), hbm(), hbm(), vmem(), vmem(), vmem()],
        out_specs=vmem(),
        scratch_shapes=[
            pltpu.VMEM((occupied, virt_all), jnp.bfloat16),
            pltpu.VMEM((2 * functions * ROWS, virt_all), jnp.bfloat16),
            pltpu.SemaphoreType.DMA((2 * functions,)),
        ],
        compiler_params=pltpu.CompilerParams(vmem_limit_bytes=52 << 20),
        cost_estimate=pl.CostEstimate(flops=flops, bytes_accessed=8 << 20, transcendentals=0),
        name="terms",
    )(both, vv_factors, vv_peer, screened_held, screened_peer, ov_held)

    terms, occ_energy, virt_energy, occ_order, virt_order = lax.optimization_barrier(
        (terms, occ_energy, virt_energy, occ_order, virt_order)
    )
    terms = lax.all_to_all(terms, WINDOW, 0, 0, tiled=True, axis_index_groups=[window])

    base = level_part(trials, occ_energy, virt_energy, occ_order, virt_order, row_offset, row_share)
    return pl.pallas_call(
        finish_kernel,
        out_shape=jax.ShapeDtypeStruct((row_share, virt), jnp.float32),
        in_specs=[vmem()] * 2,
        out_specs=vmem(),
        compiler_params=pltpu.CompilerParams(vmem_limit_bytes=8 << 20),
        name="finish",
    )(terms, base)


def solution(mesh):
    torus = Mesh(
        mesh.devices.reshape(2, 4, 4, mesh.shape["aux"], mesh.shape["grp"]),
        ("half", "x", "y", "aux", "grp"),
    )
    placed = (
        P(None, VROW),
        P(WINDOW, VROW, None),
        P(WINDOW, None, None),
        P(WINDOW, VROW, None),
        P(),
        P(),
        P(),
        P(VROW),
    )

    return jax.shard_map(on_device, mesh=torus, in_specs=placed, out_specs=P(WINDOW, VROW), check_vma=False)
```

```python
import jax
import jax.numpy as jnp
from jax import lax
from jax.experimental import pallas as pl
from jax.experimental.pallas import tpu as pltpu
from jax.sharding import Mesh
from jax.sharding import PartitionSpec as P

VROW = ("half", "x", "y")
PLANE = ("x", "y")
WINDOW = ("aux", "grp")
LANES = 128
ROWS = 128
SUBLANES = 8
PIECES = 3


def vmem():
    return pl.BlockSpec(memory_space=pltpu.VMEM)


def hbm():
    return pl.BlockSpec(memory_space=pltpu.HBM)


def in_pieces(values):
    pieces = []
    for _ in range(PIECES):
        piece = values.astype(jnp.bfloat16).astype(jnp.float32)
        pieces.append(piece)
        values = values - piece
    return pieces


def window_order(count):
    chips = count // 2
    middle = sorted(range(chips), key=lambda a: abs(2 * a + 1 - chips))
    listed = []
    for k in range(0, chips, 2):
        pair = middle[k : k + 2]
        listed += [2 * a + 1 for a in pair] + [2 * a for a in pair]
    return listed


def plane_order(count):
    first = 2 * count // 3
    return [first, *(place for place in range(count) if place != first)]


def pack_kernel(trials_hbm, ov_hbm, screened_hbm, block_ref, ov_ref, screened_ref, trials_ref, sems):
    copies = [
        pltpu.make_async_copy(trials_hbm, trials_ref, sems.at[0]),
        pltpu.make_async_copy(ov_hbm, ov_ref, sems.at[1]),
        pltpu.make_async_copy(screened_hbm, screened_ref, sems.at[2]),
    ]
    for copy in copies:
        copy.start()
    for copy in copies[:2]:
        copy.wait()
    core = lax.axis_index("grp")
    row = (lax.axis_index("half") * lax.axis_size("x") + lax.axis_index("x")) * lax.axis_size("y") + lax.axis_index("y")
    functions, occupied, virt = ov_ref.shape
    count = trials_ref.shape[0] // occupied
    spare = LANES - virt
    split = [trials_ref[pl.ds(t * occupied, occupied), :].astype(jnp.float32) for t in range(count)]
    factors = [ov_ref[q].astype(jnp.float32) for q in range(functions)]
    sums = [jnp.sum(factors[q] * split[t], axis=0, keepdims=True) for t in range(count) for q in range(functions)]
    sums = jnp.sum(jnp.concatenate(sums, axis=0), axis=1, keepdims=True)
    carried = PIECES * sums.shape[0]
    column = jnp.concatenate([*in_pieces(sums), jnp.zeros((occupied - carried, 1), jnp.float32)], axis=0)
    own = jnp.where(core == 0, split[0], split[1])
    wide = jnp.concatenate([own, jnp.broadcast_to(column, (occupied, spare))], axis=1)
    turn = lax.rem(row * virt, LANES)
    block_ref[...] = pltpu.roll(wide, turn, 1).astype(jnp.bfloat16)
    copies[2].wait()


def hold_kernel(vv_hbm, screened_ref, joint_ref, sems):
    functions, virt, _ = vv_hbm.shape
    copies = [
        pltpu.make_async_copy(vv_hbm.at[q], joint_ref.at[q, pl.ds(0, virt), :], sems.at[q]) for q in range(functions)
    ]
    for copy in copies:
        copy.start()
    occupied = screened_ref.shape[1]
    for q in range(functions):
        for k in range(occupied // SUBLANES):
            strip = screened_ref[q, pl.ds(k * SUBLANES, SUBLANES), :]
            joint_ref[q, pl.ds(virt, SUBLANES), pl.ds(k * LANES, occupied)] = strip

    for copy in copies:
        copy.wait()


def energy_part(trials_ref, occ_ref, virt_ref, occ_at_ref, virt_at_ref, base_ref):
    virt, occupied = base_ref.shape[1], occ_ref.shape[1]
    share = base_ref.shape[0]
    place = lax.axis_index("aux") * lax.axis_size("grp") + lax.axis_index("grp")
    own = trials_ref[...].astype(jnp.float32)
    rows = own[:share]
    for w in range(1, own.shape[0] // share):
        rows = jnp.where(place == w, own[w * share : (w + 1) * share], rows)

    pad = jnp.zeros((1, LANES - virt), jnp.int32)
    at = jnp.broadcast_to(jnp.concatenate([virt_at_ref[...], pad], axis=1), (SUBLANES, LANES))
    group, lane_at = at // LANES, at % LANES
    sublane = lax.broadcasted_iota(jnp.int32, (SUBLANES, LANES), 0)
    levels = jnp.zeros((SUBLANES, LANES), jnp.float32)
    count = virt_ref.shape[0]
    for k in range(0, count, SUBLANES):
        size = min(SUBLANES, count - k)
        table = virt_ref[pl.ds(k, size), :]
        if size < SUBLANES:
            table = jnp.concatenate([table, jnp.zeros((SUBLANES - size, LANES), jnp.float32)], axis=0)
        found = jnp.take_along_axis(table, lane_at, axis=1)
        levels = levels + jnp.where(sublane + k == group, found, 0.0)
    levels = jnp.sum(levels, axis=0, keepdims=True)[:, :virt]

    lane = lax.broadcasted_iota(jnp.int32, (share, occupied), 1)
    wanted = lax.rem(place * share, occupied) + lax.broadcasted_iota(jnp.int32, (share, occupied), 0)
    entry = jnp.sum(jnp.where(lane == wanted, occ_at_ref[...].astype(jnp.float32), 0.0), axis=1, keepdims=True)
    picked = lane.astype(jnp.float32) == entry
    lower = jnp.sum(jnp.where(picked, occ_ref[...], 0.0), axis=1, keepdims=True)
    base_ref[...] = (levels - lower) * rows


def term_kernel(plane, window, both_ref, joint_ref, peer_ref, ov_ref, *refs):
    *level_refs, out_ref, base_ref, whole_ref = refs
    energy_part(*level_refs, base_ref)
    core = lax.axis_index("grp")
    half = lax.axis_index("half")
    functions, occupied, virt = ov_ref.shape
    blocks = both_ref.shape[0]
    spare = LANES - virt
    tiles = blocks * virt // LANES
    entries = out_ref.shape[0] * out_ref.shape[1] // occupied * functions
    lanes = lax.broadcasted_iota(jnp.int32, (occupied, LANES), 1)
    few = lax.broadcasted_iota(jnp.int32, (PIECES * entries, LANES), 1)
    gathered = jnp.zeros((PIECES * entries, LANES), jnp.float32)
    for side in range(2):
        start = jnp.where(half == side, 0, tiles * LANES)
        held = both_ref[plane.index(0), side].astype(jnp.float32)
        for j in range(blocks):
            free = virt - spare * j
            picked = (few >= free) & (few < free + spare)
            gathered = gathered + jnp.where(picked, held[: PIECES * entries], 0.0)
            if j < tiles:
                after = both_ref[plane.index(j + 1), side].astype(jnp.float32)
                tile = jnp.where(lanes < free, held, after).astype(jnp.bfloat16)
                whole_ref[:, pl.ds(pl.multiple_of(start + j * LANES, LANES), LANES)] = tile
                held = after
    pair = jnp.sum(gathered, axis=1, keepdims=True) * (2.0 / spare)
    pair = sum(pair[k * entries : (k + 1) * entries] for k in range(PIECES))

    mine = jnp.zeros((occupied, virt), jnp.float32)
    other = jnp.zeros((occupied, virt), jnp.float32)
    for q in range(functions):
        factors = ov_ref[q].astype(jnp.float32)
        first, second = pair[q : q + 1], pair[functions + q : functions + q + 1]
        mine = mine + factors * jnp.where(core == 0, first, second)
        other = other + factors * jnp.where(core == 0, second, first)

    turned = jnp.zeros((virt, occupied), jnp.float32)
    for ref in (joint_ref, peer_ref):
        factor = ref[...].reshape(functions * ROWS, whole_ref.shape[1])
        image = lax.dot_general(factor, whole_ref[...], (((1,), (1,)), ((), ())), preferred_element_type=jnp.float32)
        image = image.astype(jnp.bfloat16)
        for q in range(functions):
            strips = [
                ref[q, pl.ds(virt, SUBLANES), pl.ds(k * LANES, occupied)].astype(jnp.float32)
                for k in range(occupied // SUBLANES)
            ]
            screen = jnp.concatenate(strips, axis=0).astype(jnp.bfloat16)
            turned = turned + jnp.dot(image[q * ROWS : q * ROWS + virt], screen, preferred_element_type=jnp.float32)
    mine = mine - turned.T

    share = out_ref.shape[1]
    per = occupied // share
    places = [window.index(w) for w in range(len(window))]
    for m in range(per):
        low, high = places[m], places[per + m]
        rows = slice(m * share, (m + 1) * share)
        out_ref[jnp.where(core == 0, low, high)] = mine[rows].astype(out_ref.dtype)
        out_ref[jnp.where(core == 0, high, low)] = other[rows].astype(out_ref.dtype)


def finish_kernel(terms_ref, base_ref, out_ref):
    total = base_ref[...]
    for place in range(terms_ref.shape[0]):
        total = total + terms_ref[place].astype(jnp.float32)
    out_ref[...] = total


def on_device(trials, vv_factors, screened, ov_factors, occ_energy, virt_energy, occ_order, virt_order):
    groups = lax.axis_size(WINDOW)
    rows_all, virt = trials.shape
    occupied = occ_energy.shape[0]
    functions, _, virt_all = vv_factors.shape
    row_share = rows_all // groups
    peers = lax.axis_size(PLANE)
    window = window_order(groups)
    plane = plane_order(peers)
    cores = [(0, 1), (1, 0)]

    ov_rows = jnp.swapaxes(ov_factors, 1, 2)
    block, ov_held, screened_held = pl.pallas_call(
        pack_kernel,
        out_shape=(
            jax.ShapeDtypeStruct((occupied, LANES), jnp.bfloat16),
            jax.ShapeDtypeStruct(ov_rows.shape, jnp.bfloat16),
            jax.ShapeDtypeStruct(screened.shape, jnp.bfloat16),
        ),
        in_specs=[hbm()] * 3,
        out_specs=(vmem(),) * 3,
        scratch_shapes=[pltpu.VMEM(trials.shape, jnp.bfloat16), pltpu.SemaphoreType.DMA((3,))],
        compiler_params=pltpu.CompilerParams(vmem_limit_bytes=54960 << 10),
        cost_estimate=pl.CostEstimate(flops=2 * 10**10, bytes_accessed=10**6, transcendentals=0),
        name="pack",
    )(trials, ov_rows, screened)

    far = lax.ppermute(block, "half", cores)

    joint = pl.pallas_call(
        hold_kernel,
        out_shape=jax.ShapeDtypeStruct((functions, ROWS, virt_all), jnp.bfloat16),
        in_specs=[hbm(), vmem()],
        out_specs=vmem(),
        scratch_shapes=[pltpu.SemaphoreType.DMA((functions,))],
        compiler_params=pltpu.CompilerParams(vmem_limit_bytes=8192 << 10),
        cost_estimate=pl.CostEstimate(flops=10**8, bytes_accessed=8 << 20, transcendentals=0),
        name="hold",
    )(vv_factors, screened_held)
    joint_peer = lax.ppermute(joint, "grp", cores)

    both = jnp.broadcast_to(jnp.stack([block, far])[None], (peers, 2, occupied, LANES))
    both = lax.all_to_all(both, PLANE, 0, 0, tiled=True, axis_index_groups=[plane])

    flops = 2 * 2 * functions * virt * virt_all * occupied
    terms, base = pl.pallas_call(
        lambda *refs: term_kernel(plane, window, *refs),
        out_shape=(
            jax.ShapeDtypeStruct((groups, row_share, virt), jnp.bfloat16),
            jax.ShapeDtypeStruct((row_share, virt), jnp.float32),
        ),
        in_specs=[vmem()] * 9,
        out_specs=(vmem(),) * 2,
        scratch_shapes=[pltpu.VMEM((occupied, virt_all), jnp.bfloat16)],
        compiler_params=pltpu.CompilerParams(vmem_limit_bytes=8192 << 10),
        cost_estimate=pl.CostEstimate(flops=flops, bytes_accessed=8 << 20, transcendentals=0),
        name="terms",
    )(
        both,
        joint,
        joint_peer,
        ov_held,
        trials,
        occ_energy.reshape(1, -1),
        virt_energy.reshape(-1, LANES),
        occ_order.reshape(1, -1),
        virt_order.reshape(1, -1),
    )

    terms = lax.all_to_all(terms, WINDOW, 0, 0, tiled=True, axis_index_groups=[window])

    return pl.pallas_call(
        finish_kernel,
        out_shape=jax.ShapeDtypeStruct((row_share, virt), jnp.float32),
        in_specs=[vmem()] * 2,
        out_specs=vmem(),
        compiler_params=pltpu.CompilerParams(vmem_limit_bytes=8 << 20),
        name="finish",
    )(terms, base)


def solution(mesh):
    torus = Mesh(
        mesh.devices.reshape(2, 4, 4, mesh.shape["aux"], mesh.shape["grp"]),
        ("half", "x", "y", "aux", "grp"),
    )
    placed = (
        P(None, VROW),
        P(WINDOW, VROW, None),
        P(WINDOW, None, None),
        P(WINDOW, VROW, None),
        P(),
        P(),
        P(),
        P(VROW),
    )

    return jax.shard_map(on_device, mesh=torus, in_specs=placed, out_specs=P(WINDOW, VROW), check_vma=False)
```

```python
import jax
import jax.numpy as jnp
from jax import lax
from jax.experimental import pallas as pl
from jax.experimental.pallas import tpu as pltpu
from jax.sharding import Mesh
from jax.sharding import PartitionSpec as P

VROW = ("half", "x", "y")
PLANE = ("x", "y")
WINDOW = ("aux", "grp")
LANES = 128
ROWS = 128
SUBLANES = 8
PIECES = 3


def vmem():
    return pl.BlockSpec(memory_space=pltpu.VMEM)


def hbm():
    return pl.BlockSpec(memory_space=pltpu.HBM)


def in_pieces(values):
    pieces = []
    for _ in range(PIECES):
        piece = values.astype(jnp.bfloat16).astype(jnp.float32)
        pieces.append(piece)
        values = values - piece
    return pieces


def window_order(count):
    chips = count // 2
    middle = sorted(range(chips), key=lambda a: abs(2 * a + 1 - chips))
    listed = []
    for k in range(0, chips, 2):
        pair = middle[k : k + 2]
        listed += [2 * a + 1 for a in pair] + [2 * a for a in pair]
    return listed


def plane_order(count):
    first = 2 * count // 3
    return [first, *(place for place in range(count) if place != first)]


def pack_kernel(trials_hbm, ov_hbm, block_ref, trials_ref, ov_ref, sems):
    copies = [
        pltpu.make_async_copy(trials_hbm, trials_ref, sems.at[0]),
        pltpu.make_async_copy(ov_hbm, ov_ref, sems.at[1]),
    ]
    for copy in copies:
        copy.start()
    for copy in copies:
        copy.wait()
    core = lax.axis_index("grp")
    row = (lax.axis_index("half") * lax.axis_size("x") + lax.axis_index("x")) * lax.axis_size("y") + lax.axis_index("y")
    functions, occupied, virt = ov_ref.shape
    count = trials_ref.shape[0] // occupied
    spare = LANES - virt
    split = [trials_ref[pl.ds(t * occupied, occupied), :].astype(jnp.float32) for t in range(count)]
    factors = [ov_ref[q].astype(jnp.float32) for q in range(functions)]
    sums = [jnp.sum(factors[q] * split[t], axis=0, keepdims=True) for t in range(count) for q in range(functions)]
    sums = jnp.sum(jnp.concatenate(sums, axis=0), axis=1, keepdims=True)
    carried = PIECES * sums.shape[0]
    column = jnp.concatenate([*in_pieces(sums), jnp.zeros((occupied - carried, 1), jnp.float32)], axis=0)
    own = jnp.where(core == 0, split[0], split[1])
    wide = jnp.concatenate([own, jnp.broadcast_to(column, (occupied, spare))], axis=1)
    turn = lax.rem(row * virt, LANES)
    block_ref[...] = pltpu.roll(wide, turn, 1).astype(jnp.bfloat16)


def hold_kernel(vv_hbm, screened_ref, joint_ref, sems):
    functions, virt, _ = vv_hbm.shape
    copies = [
        pltpu.make_async_copy(vv_hbm.at[q], joint_ref.at[q, pl.ds(0, virt), :], sems.at[q]) for q in range(functions)
    ]
    for copy in copies:
        copy.start()
    occupied = screened_ref.shape[1]
    for q in range(functions):
        for k in range(occupied // SUBLANES):
            strip = screened_ref[q, pl.ds(k * SUBLANES, SUBLANES), :]
            joint_ref[q, pl.ds(virt, SUBLANES), pl.ds(k * LANES, occupied)] = strip

    for copy in copies:
        copy.wait()


def energy_part(trials_ref, occ_ref, virt_ref, occ_at_ref, virt_at_ref, base_ref):
    virt, occupied = base_ref.shape[1], occ_ref.shape[1]
    share = base_ref.shape[0]
    place = lax.axis_index("aux") * lax.axis_size("grp") + lax.axis_index("grp")
    own = trials_ref[...].astype(jnp.float32)
    rows = own[:share]
    for w in range(1, own.shape[0] // share):
        rows = jnp.where(place == w, own[w * share : (w + 1) * share], rows)

    pad = jnp.zeros((1, LANES - virt), jnp.int32)
    at = jnp.broadcast_to(jnp.concatenate([virt_at_ref[...], pad], axis=1), (SUBLANES, LANES))
    group, lane_at = at // LANES, at % LANES
    sublane = lax.broadcasted_iota(jnp.int32, (SUBLANES, LANES), 0)
    levels = jnp.zeros((SUBLANES, LANES), jnp.float32)
    count = virt_ref.shape[0]
    for k in range(0, count, SUBLANES):
        size = min(SUBLANES, count - k)
        table = virt_ref[pl.ds(k, size), :]
        if size < SUBLANES:
            table = jnp.concatenate([table, jnp.zeros((SUBLANES - size, LANES), jnp.float32)], axis=0)
        found = jnp.take_along_axis(table, lane_at, axis=1)
        levels = levels + jnp.where(sublane + k == group, found, 0.0)
    levels = jnp.sum(levels, axis=0, keepdims=True)[:, :virt]

    lane = lax.broadcasted_iota(jnp.int32, (share, occupied), 1)
    wanted = lax.rem(place * share, occupied) + lax.broadcasted_iota(jnp.int32, (share, occupied), 0)
    entry = jnp.sum(jnp.where(lane == wanted, occ_at_ref[...].astype(jnp.float32), 0.0), axis=1, keepdims=True)
    picked = lane.astype(jnp.float32) == entry
    lower = jnp.sum(jnp.where(picked, occ_ref[...], 0.0), axis=1, keepdims=True)
    base_ref[...] = (levels - lower) * rows


def term_kernel(plane, window, both_ref, joint_ref, peer_ref, ov_ref, *refs):
    *level_refs, out_ref, base_ref, whole_ref = refs
    core = lax.axis_index("grp")
    half = lax.axis_index("half")
    functions, occupied, virt = ov_ref.shape
    blocks = both_ref.shape[0]
    spare = LANES - virt
    tiles = blocks * virt // LANES
    entries = out_ref.shape[0] * out_ref.shape[1] // occupied * functions
    lanes = lax.broadcasted_iota(jnp.int32, (occupied, LANES), 1)
    few = lax.broadcasted_iota(jnp.int32, (PIECES * entries, LANES), 1)
    gathered = jnp.zeros((PIECES * entries, LANES), jnp.float32)
    for side in range(2):
        start = jnp.where(half == side, 0, tiles * LANES)
        held = both_ref[plane.index(0), side].astype(jnp.float32)
        for j in range(blocks):
            free = virt - spare * j
            picked = (few >= free) & (few < free + spare)
            gathered = gathered + jnp.where(picked, held[: PIECES * entries], 0.0)
            if j < tiles:
                after = both_ref[plane.index(j + 1), side].astype(jnp.float32)
                tile = jnp.where(lanes < free, held, after).astype(jnp.bfloat16)
                whole_ref[:, pl.ds(pl.multiple_of(start + j * LANES, LANES), LANES)] = tile
                held = after
    pair = jnp.sum(gathered, axis=1, keepdims=True) * (2.0 / spare)
    pair = sum(pair[k * entries : (k + 1) * entries] for k in range(PIECES))

    def contracted(ref):
        factor = ref[...].reshape(functions * ROWS, whole_ref.shape[1])
        image = lax.dot_general(factor, whole_ref[...], (((1,), (1,)), ((), ())), preferred_element_type=jnp.float32)
        return image.astype(jnp.bfloat16)

    def screened(image, ref):
        total = jnp.zeros((virt, occupied), jnp.float32)
        for q in range(functions):
            strips = [
                ref[q, pl.ds(virt, SUBLANES), pl.ds(k * LANES, occupied)].astype(jnp.float32)
                for k in range(occupied // SUBLANES)
            ]
            screen = jnp.concatenate(strips, axis=0).astype(jnp.bfloat16)
            total = total + jnp.dot(image[q * ROWS : q * ROWS + virt], screen, preferred_element_type=jnp.float32)
        return total

    own = contracted(joint_ref)
    peer = contracted(peer_ref)
    turned = screened(own, joint_ref)
    mine = jnp.zeros((occupied, virt), jnp.float32)
    other = jnp.zeros((occupied, virt), jnp.float32)
    for q in range(functions):
        factors = ov_ref[q].astype(jnp.float32)
        first, second = pair[q : q + 1], pair[functions + q : functions + q + 1]
        mine = mine + factors * jnp.where(core == 0, first, second)
        other = other + factors * jnp.where(core == 0, second, first)

    energy_part(*level_refs, base_ref)
    turned = turned + screened(peer, peer_ref)
    mine = mine - turned.T

    share = out_ref.shape[1]
    per = occupied // share
    places = [window.index(w) for w in range(len(window))]
    for m in range(per):
        low, high = places[m], places[per + m]
        rows = slice(m * share, (m + 1) * share)
        out_ref[jnp.where(core == 0, low, high)] = mine[rows].astype(out_ref.dtype)
        out_ref[jnp.where(core == 0, high, low)] = other[rows].astype(out_ref.dtype)


def finish_kernel(terms_ref, base_ref, out_ref):
    total = base_ref[...]
    for place in range(terms_ref.shape[0]):
        total = total + terms_ref[place].astype(jnp.float32)
    out_ref[...] = total


def on_device(trials, vv_factors, screened, ov_factors, occ_energy, virt_energy, occ_order, virt_order):
    groups = lax.axis_size(WINDOW)
    rows_all, virt = trials.shape
    occupied = occ_energy.shape[0]
    functions, _, virt_all = vv_factors.shape
    row_share = rows_all // groups
    peers = lax.axis_size(PLANE)
    window = window_order(groups)
    plane = plane_order(peers)
    cores = [(0, 1), (1, 0)]

    ov_rows = jnp.swapaxes(ov_factors, 1, 2)
    block = pl.pallas_call(
        pack_kernel,
        out_shape=jax.ShapeDtypeStruct((occupied, LANES), jnp.bfloat16),
        in_specs=[hbm()] * 2,
        out_specs=vmem(),
        scratch_shapes=[
            pltpu.VMEM(trials.shape, jnp.bfloat16),
            pltpu.VMEM(ov_rows.shape, jnp.bfloat16),
            pltpu.SemaphoreType.DMA((2,)),
        ],
        compiler_params=pltpu.CompilerParams(vmem_limit_bytes=55200 << 10),
        cost_estimate=pl.CostEstimate(flops=2 * 10**10, bytes_accessed=10**6, transcendentals=0),
        name="pack",
    )(trials, ov_rows)

    far = lax.ppermute(block, "half", cores)

    joint = pl.pallas_call(
        hold_kernel,
        out_shape=jax.ShapeDtypeStruct((functions, ROWS, virt_all), jnp.bfloat16),
        in_specs=[hbm(), vmem()],
        out_specs=vmem(),
        scratch_shapes=[pltpu.SemaphoreType.DMA((functions,))],
        compiler_params=pltpu.CompilerParams(vmem_limit_bytes=8192 << 10),
        cost_estimate=pl.CostEstimate(flops=10**8, bytes_accessed=8 << 20, transcendentals=0),
        name="hold",
    )(vv_factors, screened)
    joint_peer = lax.ppermute(joint, "grp", cores)

    both = jnp.broadcast_to(jnp.stack([block, far])[None], (peers, 2, occupied, LANES))
    both = lax.all_to_all(both, PLANE, 0, 0, tiled=True, axis_index_groups=[plane])

    flops = 2 * 2 * functions * virt * virt_all * occupied
    terms, base = pl.pallas_call(
        lambda *refs: term_kernel(plane, window, *refs),
        out_shape=(
            jax.ShapeDtypeStruct((groups, row_share, virt), jnp.bfloat16),
            jax.ShapeDtypeStruct((row_share, virt), jnp.float32),
        ),
        in_specs=[vmem()] * 9,
        out_specs=(vmem(),) * 2,
        scratch_shapes=[pltpu.VMEM((occupied, virt_all), jnp.bfloat16)],
        compiler_params=pltpu.CompilerParams(vmem_limit_bytes=8192 << 10),
        cost_estimate=pl.CostEstimate(flops=flops, bytes_accessed=8 << 20, transcendentals=0),
        name="terms",
    )(
        both,
        joint,
        joint_peer,
        ov_rows,
        trials,
        occ_energy.reshape(1, -1),
        virt_energy.reshape(-1, LANES),
        occ_order.reshape(1, -1),
        virt_order.reshape(1, -1),
    )

    terms = lax.all_to_all(terms, WINDOW, 0, 0, tiled=True, axis_index_groups=[window])

    return pl.pallas_call(
        finish_kernel,
        out_shape=jax.ShapeDtypeStruct((row_share, virt), jnp.float32),
        in_specs=[vmem()] * 2,
        out_specs=vmem(),
        compiler_params=pltpu.CompilerParams(vmem_limit_bytes=8 << 20),
        name="finish",
    )(terms, base)


def solution(mesh):
    torus = Mesh(
        mesh.devices.reshape(2, 4, 4, mesh.shape["aux"], mesh.shape["grp"]),
        ("half", "x", "y", "aux", "grp"),
    )
    placed = (
        P(None, VROW),
        P(WINDOW, VROW, None),
        P(WINDOW, None, None),
        P(WINDOW, VROW, None),
        P(),
        P(),
        P(),
        P(VROW),
    )

    return jax.shard_map(on_device, mesh=torus, in_specs=placed, out_specs=P(WINDOW, VROW), check_vma=False)
```

```python
import jax
import jax.numpy as jnp
from jax import lax
from jax.experimental import pallas as pl
from jax.experimental.pallas import tpu as pltpu
from jax.sharding import Mesh
from jax.sharding import PartitionSpec as P

VROW = ("half", "x", "y")
PLANE = ("x", "y")
WINDOW = ("aux", "grp")
LANES = 128
ROWS = 128
SUBLANES = 8
PIECES = 3


def vmem():
    return pl.BlockSpec(memory_space=pltpu.VMEM)


def hbm():
    return pl.BlockSpec(memory_space=pltpu.HBM)


def in_pieces(values):
    pieces = []
    for _ in range(PIECES):
        piece = values.astype(jnp.bfloat16).astype(jnp.float32)
        pieces.append(piece)
        values = values - piece
    return pieces


def window_order(count):
    chips = count // 2
    middle = sorted(range(chips), key=lambda a: abs(2 * a + 1 - chips))
    listed = []
    for k in range(0, chips, 2):
        pair = middle[k : k + 2]
        listed += [2 * a + 1 for a in pair] + [2 * a for a in pair]
    first = count // 2 + 1
    return [first, *(place for place in listed if place != first)]


def plane_order(count):
    first = count // 3
    return [first, *(place for place in range(count) if place != first)]


def pack_kernel(trials_hbm, ov_hbm, block_ref, trials_ref, ov_ref, sems):
    copies = [
        pltpu.make_async_copy(trials_hbm, trials_ref, sems.at[0]),
        pltpu.make_async_copy(ov_hbm, ov_ref, sems.at[1]),
    ]
    for copy in copies:
        copy.start()
    for copy in copies:
        copy.wait()
    core = lax.axis_index("grp")
    row = (lax.axis_index("half") * lax.axis_size("x") + lax.axis_index("x")) * lax.axis_size("y") + lax.axis_index("y")
    functions, occupied, virt = ov_ref.shape
    count = trials_ref.shape[0] // occupied
    spare = LANES - virt
    split = [trials_ref[pl.ds(t * occupied, occupied), :].astype(jnp.float32) for t in range(count)]
    factors = [ov_ref[q].astype(jnp.float32) for q in range(functions)]
    sums = [jnp.sum(factors[q] * split[t], axis=0, keepdims=True) for t in range(count) for q in range(functions)]
    sums = jnp.sum(jnp.concatenate(sums, axis=0), axis=1, keepdims=True)
    carried = PIECES * sums.shape[0]
    column = jnp.concatenate([*in_pieces(sums), jnp.zeros((occupied - carried, 1), jnp.float32)], axis=0)
    own = jnp.where(core == 0, split[0], split[1])
    wide = jnp.concatenate([own, jnp.broadcast_to(column, (occupied, spare))], axis=1)
    turn = lax.rem(row * virt, LANES)
    block_ref[...] = pltpu.roll(wide, turn, 1).astype(jnp.bfloat16)


def hold_kernel(vv_hbm, screened_ref, joint_ref, sems):
    functions, virt, _ = vv_hbm.shape
    copies = [
        pltpu.make_async_copy(vv_hbm.at[q], joint_ref.at[q, pl.ds(0, virt), :], sems.at[q]) for q in range(functions)
    ]
    for copy in copies:
        copy.start()
    occupied = screened_ref.shape[1]
    for q in range(functions):
        for k in range(occupied // SUBLANES):
            strip = screened_ref[q, pl.ds(k * SUBLANES, SUBLANES), :]
            joint_ref[q, pl.ds(virt, SUBLANES), pl.ds(k * LANES, occupied)] = strip

    for copy in copies:
        copy.wait()


def energy_part(trials_ref, occ_ref, virt_ref, occ_at_ref, virt_at_ref, base_ref):
    virt, occupied = base_ref.shape[1], occ_ref.shape[1]
    share = base_ref.shape[0]
    place = lax.axis_index("aux") * lax.axis_size("grp") + lax.axis_index("grp")
    own = trials_ref[...].astype(jnp.float32)
    rows = own[:share]
    for w in range(1, own.shape[0] // share):
        rows = jnp.where(place == w, own[w * share : (w + 1) * share], rows)

    pad = jnp.zeros((1, LANES - virt), jnp.int32)
    at = jnp.broadcast_to(jnp.concatenate([virt_at_ref[...], pad], axis=1), (SUBLANES, LANES))
    group, lane_at = at // LANES, at % LANES
    sublane = lax.broadcasted_iota(jnp.int32, (SUBLANES, LANES), 0)
    levels = jnp.zeros((SUBLANES, LANES), jnp.float32)
    count = virt_ref.shape[0]
    for k in range(0, count, SUBLANES):
        size = min(SUBLANES, count - k)
        table = virt_ref[pl.ds(k, size), :]
        if size < SUBLANES:
            table = jnp.concatenate([table, jnp.zeros((SUBLANES - size, LANES), jnp.float32)], axis=0)
        found = jnp.take_along_axis(table, lane_at, axis=1)
        levels = levels + jnp.where(sublane + k == group, found, 0.0)
    levels = jnp.sum(levels, axis=0, keepdims=True)[:, :virt]

    lane = lax.broadcasted_iota(jnp.int32, (share, occupied), 1)
    wanted = lax.rem(place * share, occupied) + lax.broadcasted_iota(jnp.int32, (share, occupied), 0)
    entry = jnp.sum(jnp.where(lane == wanted, occ_at_ref[...].astype(jnp.float32), 0.0), axis=1, keepdims=True)
    picked = lane.astype(jnp.float32) == entry
    lower = jnp.sum(jnp.where(picked, occ_ref[...], 0.0), axis=1, keepdims=True)
    base_ref[...] = (levels - lower) * rows


def term_kernel(plane, window, both_ref, joint_ref, peer_ref, ov_ref, *refs):
    *level_refs, out_ref, base_ref, whole_ref = refs
    core = lax.axis_index("grp")
    half = lax.axis_index("half")
    functions, occupied, virt = ov_ref.shape
    blocks = both_ref.shape[0]
    spare = LANES - virt
    tiles = blocks * virt // LANES
    entries = out_ref.shape[0] * out_ref.shape[1] // occupied * functions
    lanes = lax.broadcasted_iota(jnp.int32, (occupied, LANES), 1)
    few = lax.broadcasted_iota(jnp.int32, (PIECES * entries, LANES), 1)
    gathered = jnp.zeros((PIECES * entries, LANES), jnp.float32)
    for side in range(2):
        start = jnp.where(half == side, 0, tiles * LANES)
        held = both_ref[plane.index(0), side].astype(jnp.float32)
        for j in range(blocks):
            free = virt - spare * j
            picked = (few >= free) & (few < free + spare)
            gathered = gathered + jnp.where(picked, held[: PIECES * entries], 0.0)
            if j < tiles:
                after = both_ref[plane.index(j + 1), side].astype(jnp.float32)
                tile = jnp.where(lanes < free, held, after).astype(jnp.bfloat16)
                whole_ref[:, pl.ds(pl.multiple_of(start + j * LANES, LANES), LANES)] = tile
                held = after
    pair = jnp.sum(gathered, axis=1, keepdims=True) * (2.0 / spare)
    pair = sum(pair[k * entries : (k + 1) * entries] for k in range(PIECES))

    def contracted(ref):
        factor = ref[...].reshape(functions * ROWS, whole_ref.shape[1])
        image = lax.dot_general(factor, whole_ref[...], (((1,), (1,)), ((), ())), preferred_element_type=jnp.float32)
        return image.astype(jnp.bfloat16)

    def screened(image, ref):
        total = jnp.zeros((virt, occupied), jnp.float32)
        for q in range(functions):
            strips = [
                ref[q, pl.ds(virt, SUBLANES), pl.ds(k * LANES, occupied)].astype(jnp.float32)
                for k in range(occupied // SUBLANES)
            ]
            screen = jnp.concatenate(strips, axis=0).astype(jnp.bfloat16)
            total = total + jnp.dot(image[q * ROWS : q * ROWS + virt], screen, preferred_element_type=jnp.float32)
        return total

    own = contracted(joint_ref)
    peer = contracted(peer_ref)
    turned = screened(own, joint_ref)
    mine = jnp.zeros((occupied, virt), jnp.float32)
    other = jnp.zeros((occupied, virt), jnp.float32)
    for q in range(functions):
        factors = ov_ref[q].astype(jnp.float32)
        first, second = pair[q : q + 1], pair[functions + q : functions + q + 1]
        mine = mine + factors * jnp.where(core == 0, first, second)
        other = other + factors * jnp.where(core == 0, second, first)

    energy_part(*level_refs, base_ref)
    turned = turned + screened(peer, peer_ref)
    mine = mine - turned.T

    share = out_ref.shape[1]
    per = occupied // share
    places = [window.index(w) for w in range(len(window))]
    for m in range(per):
        low, high = places[m], places[per + m]
        rows = slice(m * share, (m + 1) * share)
        out_ref[jnp.where(core == 0, low, high)] = mine[rows].astype(out_ref.dtype)
        out_ref[jnp.where(core == 0, high, low)] = other[rows].astype(out_ref.dtype)


def finish_kernel(terms_ref, base_ref, out_ref):
    total = base_ref[...]
    for place in range(terms_ref.shape[0]):
        total = total + terms_ref[place].astype(jnp.float32)
    out_ref[...] = total


def on_device(trials, vv_factors, screened, ov_factors, occ_energy, virt_energy, occ_order, virt_order):
    groups = lax.axis_size(WINDOW)
    rows_all, virt = trials.shape
    occupied = occ_energy.shape[0]
    functions, _, virt_all = vv_factors.shape
    row_share = rows_all // groups
    peers = lax.axis_size(PLANE)
    window = window_order(groups)
    plane = plane_order(peers)
    cores = [(0, 1), (1, 0)]

    ov_rows = jnp.swapaxes(ov_factors, 1, 2)
    block = pl.pallas_call(
        pack_kernel,
        out_shape=jax.ShapeDtypeStruct((occupied, LANES), jnp.bfloat16),
        in_specs=[hbm()] * 2,
        out_specs=vmem(),
        scratch_shapes=[
            pltpu.VMEM(trials.shape, jnp.bfloat16),
            pltpu.VMEM(ov_rows.shape, jnp.bfloat16),
            pltpu.SemaphoreType.DMA((2,)),
        ],
        compiler_params=pltpu.CompilerParams(vmem_limit_bytes=55200 << 10),
        cost_estimate=pl.CostEstimate(flops=2 * 10**10, bytes_accessed=10**6, transcendentals=0),
        name="pack",
    )(trials, ov_rows)

    far = lax.ppermute(block, "half", cores)

    joint = pl.pallas_call(
        hold_kernel,
        out_shape=jax.ShapeDtypeStruct((functions, ROWS, virt_all), jnp.bfloat16),
        in_specs=[hbm(), vmem()],
        out_specs=vmem(),
        scratch_shapes=[pltpu.SemaphoreType.DMA((functions,))],
        compiler_params=pltpu.CompilerParams(vmem_limit_bytes=8192 << 10),
        cost_estimate=pl.CostEstimate(flops=10**8, bytes_accessed=8 << 20, transcendentals=0),
        name="hold",
    )(vv_factors, screened)
    joint_peer = lax.ppermute(joint, "grp", cores)

    both = jnp.broadcast_to(jnp.stack([block, far])[None], (peers, 2, occupied, LANES))
    both = lax.all_to_all(both, PLANE, 0, 0, tiled=True, axis_index_groups=[plane])

    flops = 2 * 2 * functions * virt * virt_all * occupied
    terms, base = pl.pallas_call(
        lambda *refs: term_kernel(plane, window, *refs),
        out_shape=(
            jax.ShapeDtypeStruct((groups, row_share, virt), jnp.bfloat16),
            jax.ShapeDtypeStruct((row_share, virt), jnp.float32),
        ),
        in_specs=[vmem()] * 9,
        out_specs=(vmem(),) * 2,
        scratch_shapes=[pltpu.VMEM((occupied, virt_all), jnp.bfloat16)],
        compiler_params=pltpu.CompilerParams(vmem_limit_bytes=8192 << 10),
        cost_estimate=pl.CostEstimate(flops=flops, bytes_accessed=8 << 20, transcendentals=0),
        name="terms",
    )(
        both,
        joint,
        joint_peer,
        ov_rows,
        trials,
        occ_energy.reshape(1, -1),
        virt_energy.reshape(-1, LANES),
        occ_order.reshape(1, -1),
        virt_order.reshape(1, -1),
    )

    terms = lax.all_to_all(terms, WINDOW, 0, 0, tiled=True, axis_index_groups=[window])

    return pl.pallas_call(
        finish_kernel,
        out_shape=jax.ShapeDtypeStruct((row_share, virt), jnp.float32),
        in_specs=[vmem()] * 2,
        out_specs=vmem(),
        compiler_params=pltpu.CompilerParams(vmem_limit_bytes=8 << 20),
        name="finish",
    )(terms, base)


def solution(mesh):
    torus = Mesh(
        mesh.devices.reshape(2, 4, 4, mesh.shape["aux"], mesh.shape["grp"]),
        ("half", "x", "y", "aux", "grp"),
    )
    placed = (
        P(None, VROW),
        P(WINDOW, VROW, None),
        P(WINDOW, None, None),
        P(WINDOW, VROW, None),
        P(),
        P(),
        P(),
        P(VROW),
    )

    return jax.shard_map(on_device, mesh=torus, in_specs=placed, out_specs=P(WINDOW, VROW), check_vma=False)
```
